32 devices in a mesh: dp: 2 (over x), tp: 4 (over z), pp: 4 (over y, core).
Axes of the slice: x: 2, y: 2, z: 4, core: 2. Of those that a mesh axis runs over, the one named last changes fastest.
Arguments:
- tokens_in: bfloat16 [24, 128, 1024], P('dp'), parts along dimension 0
- targets: bfloat16 [24, 128, 1024], P('dp'), parts along dimension 0
- w_in: bfloat16 [4, 2, 1024, 4096], P('pp', None, None, 'tp')
- w_out: bfloat16 [4, 2, 4096, 1024], P('pp', None, 'tp')
Outputs:
- output 1: float32 [8, 2, 1024, 4096], P(('dp', 'pp'), None, None, 'tp'), parts along dimension 0
- output 2: float32 [8, 2, 4096, 1024], P(('dp', 'pp'), None, 'tp'), parts along dimension 0
- output 3: float32 [2], P('dp'), parts along dimension 0
There are 2 independent parts. The reference program is written for one: setup_inputs(seed, part) draws one part's arguments, and reference() takes and returns one part's arrays. A program takes and returns all parts, laid end to end along the dimension named above; an argument that names none is the same for every part.
All inputs are finite; a program needn't handle non-finite values.
Results may differ from the reference program's by a relative error of at most 0.00808713.
Values are sent between devices in bfloat16 or wider.
A program may use at most 1 GiB of HBM per device.

```python
import jax
import jax.numpy as jnp
from jax import lax

STAGES = 4
MICRO = 12
TOKENS = 128
D = 1024
FF = 4096


def setup_inputs(seed: int = 0, part: int = 0) -> dict:
    base_key = jax.random.key(seed)
    shared_key, data_base = jax.random.split(base_key)
    data_key = jax.random.fold_in(data_base, part)
    x_key, y_key = jax.random.split(data_key)
    first_key, second_key = jax.random.split(shared_key)
    n_layers = 2 * STAGES
    tokens_in = jax.random.normal(x_key, (MICRO, TOKENS, D), jnp.float32).astype(jnp.bfloat16)
    targets = (1.5 * jax.random.normal(y_key, (MICRO, TOKENS, D), jnp.float32)).astype(jnp.bfloat16)
    w_in = (jax.random.normal(first_key, (STAGES, 2, D, FF), jnp.float32) * D ** -0.5).astype(jnp.bfloat16)
    w_out = (jax.random.normal(second_key, (STAGES, 2, FF, D), jnp.float32) * (2.0 * (FF * n_layers) ** -0.5)).astype(jnp.bfloat16)
    return {"tokens_in": tokens_in, "targets": targets, "w_in": w_in, "w_out": w_out}


def reference(tokens_in, targets, w_in, w_out):
    n_layers = 2 * STAGES
    stack_in = w_in.reshape(n_layers, D, FF)
    stack_out = w_out.reshape(n_layers, FF, D)
    inv_count = 1.0 / (MICRO * TOKENS * D)

    def fwd_step(act_in, weights):
        w_first, w_second = weights
        pre_act = jnp.dot(act_in, w_first, preferred_element_type=jnp.float32).astype(jnp.bfloat16)
        post_act = jax.nn.gelu(pre_act.astype(jnp.float32)).astype(jnp.bfloat16)
        branch = jnp.dot(post_act, w_second, preferred_element_type=jnp.float32)
        act_out = (act_in.astype(jnp.float32) + branch).astype(jnp.bfloat16)
        return act_out, (act_in, pre_act, post_act)

    def bwd_step(cur_grad, layer_items):
        w_first, w_second, act_in, pre_act, post_act, acc_first, acc_second = layer_items
        back_grad = jnp.dot(cur_grad, w_second.T, preferred_element_type=jnp.float32)
        gelu_pull = jax.vjp(jax.nn.gelu, pre_act.astype(jnp.float32))[1]
        gate_grad = gelu_pull(back_grad)[0].astype(jnp.bfloat16)
        spread = jnp.dot(gate_grad, w_first.T, preferred_element_type=jnp.float32)
        prev_grad = (cur_grad.astype(jnp.float32) + spread).astype(jnp.bfloat16)
        new_first = acc_first + jnp.dot(act_in.T, gate_grad, preferred_element_type=jnp.float32)
        new_second = acc_second + jnp.dot(post_act.T, cur_grad, preferred_element_type=jnp.float32)
        return prev_grad, (new_first, new_second)

    def one_micro(loop_state, micro_pair):
        acc_first, acc_second, loss_sum = loop_state
        x_mb, y_mb = micro_pair
        y_out, saved_acts = lax.scan(fwd_step, x_mb, (stack_in, stack_out))
        error_val = y_out.astype(jnp.float32) - y_mb.astype(jnp.float32)
        out_grad = (error_val * inv_count).astype(jnp.bfloat16)
        last_grad, (acc_first, acc_second) = lax.scan(bwd_step, out_grad, (stack_in, stack_out) + saved_acts + (acc_first, acc_second), reverse=True)
        return (acc_first, acc_second, loss_sum + 0.5 * jnp.sum(error_val * error_val)), None

    init_state = (jnp.zeros((n_layers, D, FF), jnp.float32), jnp.zeros((n_layers, FF, D), jnp.float32), jnp.zeros((), jnp.float32))
    (acc_first, acc_second, loss_sum), last_ys = lax.scan(one_micro, init_state, (tokens_in, targets))
    return (acc_first.reshape(STAGES, 2, D, FF), acc_second.reshape(STAGES, 2, FF, D), (loss_sum * inv_count).reshape(1))
```

```python
import functools
import math

import jax
import jax.numpy as jnp
from jax import lax
from jax.experimental import pallas as pl
from jax.experimental.pallas import tpu as pltpu
from jax.sharding import PartitionSpec as P

BF = jnp.bfloat16
F32 = jnp.float32
NP = 4
RING = 4
GC = math.sqrt(2.0 / math.pi)
NT = (((1,), (1,)), ((), ()))
MESH = pl.DeviceIdType.MESH


def gelu_f(x):
    return x * (0.5 + 0.5 * jnp.tanh(GC * (x + 0.044715 * (x * x * x))))


def gelu_d(x):
    x2 = x * x
    th = jnp.tanh(GC * (x + 0.044715 * (x * x2)))
    return 0.5 + 0.5 * th + (0.5 * x) * (1.0 - th * th) * (GC + (3 * 0.044715 * GC) * x2)


def step_kernel(n_stage, n_tp, inv_count, x_hbm, t_hbm, w1_hbm, w2_hbm,
                a_out, d_out, g_out, z_out, loss_out,
                w1, w2, act, gbuf, zbuf, pbuf, qbuf, sbuf, obuf, own, tbuf, lacc, ltile,
                xsem, wsem, psem, qsem, ssem, oesem, oosem, ldsem, tsem, outsem, lsend, lrecv):
    n_micro, _, n_tok, dp_cols = act.shape[1:]
    hid = gbuf.shape[3]
    hb = hid // NP
    n_layer = 2 * n_stage
    stage = lax.axis_index("pp")
    z = lax.axis_index("tp")
    is_mid = (z == 1) | (z == 2)
    is_end = jnp.logical_not(is_mid)
    partner = z + 1 - 2 * lax.rem(z, 2)
    other = n_tp - 1 - z
    first = stage == 0
    last = stage == n_stage - 1
    offs = (2 * stage, 2 * stage + 1, 2 * n_layer - 2 - 2 * stage, 2 * n_layer - 1 - 2 * stage)

    def rcopy(src, dst, s_sem, r_sem, tp, pp):
        return pltpu.make_async_remote_copy(src_ref=src, dst_ref=dst, send_sem=s_sem, recv_sem=r_sem,
                                            device_id={"tp": tp, "pp": pp}, device_id_type=MESH)

    def wait_in(ref, sem):
        pltpu.make_async_copy(ref, ref, sem).wait()

    loads = []
    for k in range(2):
        loads.append(pltpu.make_async_copy(w1_hbm.at[0, k], w1.at[k], ldsem.at[k]))
        loads.append(pltpu.make_async_copy(w2_hbm.at[0, k], w2.at[k], ldsem.at[2 + k]))
    for ld in loads:
        ld.start()

    @pl.when(first)
    def _():
        @pl.loop(0, n_micro)
        def _(m):
            for c in range(NP):
                pltpu.make_async_copy(x_hbm.at[m, :, pl.ds(c * dp_cols, dp_cols)], act.at[0, m, c], xsem.at[0, m, c]).start()

    @pl.when(last & is_mid)
    def _():
        @pl.loop(0, n_micro)
        def _(m):
            for c in range(NP):
                pltpu.make_async_copy(t_hbm.at[m, :, pl.ds(c * dp_cols, dp_cols)], tbuf.at[m, c], tsem).start()

    lacc[...] = jnp.zeros_like(lacc)
    for ld in loads:
        ld.wait()

    @pl.when(last & is_mid)
    def _():
        wait_in(tbuf, tsem)

    def emit_piece(slot, m, c, part):
        @pl.when(is_end)
        def _():
            sbuf[slot, c] = part.astype(BF)
            r = lax.rem(m, RING)
            rcopy(sbuf.at[slot, c], pbuf.at[slot, r, c], ssem.at[slot], psem.at[slot, r, c], partner, stage).start()

        @pl.when(is_mid)
        def _():
            own[slot % 2, c] = part

    def load_full(ai, m):
        return jnp.concatenate([act[ai, m, c] for c in range(NP)], axis=1)

    def put_act(src_idx, m, dst, sem):
        for c in range(NP):
            pltpu.make_async_copy(act.at[src_idx, m, c],
                                  dst.at[src_idx % 2, pl.ds(m * n_tok, n_tok), pl.ds(c * dp_cols, dp_cols)], sem).start()

    def do_a(slot, m):
        fwd = slot < 2
        k = slot if fwd else 3 - slot
        ai = k if fwd else 2 + k
        r = lax.rem(m, RING)
        if slot == 0:
            for c in range(NP):
                wait_in(act.at[ai, m, c], xsem.at[0, m, c])
        elif slot == 2:
            @pl.when(jnp.logical_not(last & is_mid))
            def _():
                for c in range(NP):
                    wait_in(act.at[ai, m, c], xsem.at[1, m, c])
        else:
            @pl.when(is_end)
            def _():
                for c in range(NP):
                    wait_in(act.at[ai, m, c], wsem.at[0 if fwd else 1, r, c])

        @pl.when(is_end & (m > 0) & (jnp.logical_not(first) if slot == 3 else True))
        def _():
            wait_in(sbuf.at[slot], ssem.at[slot])

        put_act(ai, m, a_out if fwd else d_out, outsem.at[0 if fwd else 1])
        rows = pl.ds(m * n_tok, n_tok)
        if fwd:
            a = load_full(ai, m)
            for n in range(NP):
                cs = pl.ds(n * hb, hb)
                u = jnp.dot(a, w1[k, :, cs], preferred_element_type=F32).astype(BF)
                gbuf[k, m, :, cs] = u
                zbuf[k, m, :, cs] = gelu_f(u.astype(F32)).astype(BF)
            pltpu.make_async_copy(zbuf.at[k, m], z_out.at[k, rows], outsem.at[2]).start()
            zz = zbuf[k, m]
            for c in range(NP):
                emit_piece(slot, m, c, jnp.dot(zz, w2[k, :, pl.ds(c * dp_cols, dp_cols)], preferred_element_type=F32))
        else:
            d = load_full(ai, m)
            for n in range(NP):
                cs = pl.ds(n * hb, hb)
                up = lax.dot_general(d, w2[k, cs, :], NT, preferred_element_type=F32)
                gbuf[k, m, :, cs] = (gelu_d(gbuf[k, m, :, cs].astype(F32)) * up).astype(BF)
            pltpu.make_async_copy(gbuf.at[k, m], g_out.at[k, rows], outsem.at[3]).start()

            def parts():
                gg = gbuf[k, m]
                for c in range(NP):
                    emit_piece(slot, m, c, lax.dot_general(gg, w1[k, pl.ds(c * dp_cols, dp_cols), :], NT, preferred_element_type=F32))

            if slot == 3:
                pl.when(jnp.logical_not(first))(parts)
            else:
                parts()

    def do_b(slot, m):
        @pl.when(m > 0)
        def _():
            wait_in(sbuf.at[slot], ssem.at[slot])
        r = lax.rem(m, RING)
        for c in range(NP):
            wait_in(pbuf.at[slot, r, c], psem.at[slot, r, c])
            sbuf[slot, c] = (own[slot % 2, c] + pbuf[slot, r, c].astype(F32)).astype(BF)
            rcopy(sbuf.at[slot, c], qbuf.at[slot, r, c], ssem.at[slot], qsem.at[slot, r, c], other, stage).start()

    def do_c(slot, m):
        fwd = slot < 2
        k = slot if fwd else 3 - slot
        ai = k if fwd else 2 + k
        r = lax.rem(m, RING)

        @pl.when(m > 0)
        def _():
            wait_in(obuf.at[slot], oesem.at[slot])
            if slot == 1:
                @pl.when(jnp.logical_not(last))
                def _():
                    wait_in(obuf.at[slot], oosem.at[slot])
            if slot == 3:
                wait_in(obuf.at[slot], oosem.at[slot])

        for c in range(NP):
            wait_in(qbuf.at[slot, r, c], qsem.at[slot, r, c])
            h = act[ai, m, c].astype(F32) + (sbuf[slot, c].astype(F32) + qbuf[slot, r, c].astype(F32))
            h = h.astype(BF)
            if slot == 0 or slot == 2:
                di = 1 if slot == 0 else 2
                obuf[slot, c] = h
                act[di, m, c] = h
                rcopy(obuf.at[slot, c], act.at[di, m, c], oesem.at[slot], wsem.at[slot // 2, r, c], partner, stage).start()
            elif slot == 1:
                @pl.when(last)
                def _():
                    err = h.astype(F32) - tbuf[m, c].astype(F32)
                    lacc[...] += jnp.sum((err * err).reshape(n_tok // 8, 8, dp_cols), axis=0)
                    dy = (err * inv_count).astype(BF)
                    obuf[slot, c] = dy
                    act[3, m, c] = dy
                    rcopy(obuf.at[slot, c], act.at[3, m, c], oesem.at[slot], xsem.at[1, m, c], partner, stage).start()

                @pl.when(jnp.logical_not(last))
                def _():
                    obuf[slot, c] = h
                    rcopy(obuf.at[slot, c], act.at[0, m, c], oosem.at[slot], xsem.at[0, m, c], z, stage + 1).start()
                    rcopy(obuf.at[slot, c], act.at[0, m, c], oesem.at[slot], xsem.at[0, m, c], partner, stage + 1).start()
            else:
                obuf[slot, c] = h
                rcopy(obuf.at[slot, c], act.at[3, m, c], oosem.at[slot], xsem.at[1, m, c], z, stage - 1).start()
                rcopy(obuf.at[slot, c], act.at[3, m, c], oesem.at[slot], xsem.at[1, m, c], partner, stage - 1).start()

    def tick(t, carry):
        for slot in range(4):
            m = t - offs[slot]
            pl.when((m >= 0) & (m < n_micro))(functools.partial(do_a, slot, m))
            sb = (slot + 3) % 4
            mb = t - offs[sb] - (1 if slot < 1 else 0)
            ok = is_mid & (mb >= 0) & (mb < n_micro)
            if sb == 3:
                ok = ok & jnp.logical_not(first)
            pl.when(ok)(functools.partial(do_b, sb, mb))
            sc = (slot + 2) % 4
            mc = t - offs[sc] - (1 if slot < 2 else 0)
            ok = is_mid & (mc >= 0) & (mc < n_micro)
            if sc == 3:
                ok = ok & jnp.logical_not(first)
            pl.when(ok)(functools.partial(do_c, sc, mc))
        return carry

    lax.fori_loop(0, n_micro + 2 * n_layer, tick, 0)

    owner = (z == 1) & last

    @pl.when(owner)
    def _():
        ltile[...] = jnp.full(ltile.shape, jnp.sum(lacc[...]) * inv_count * 0.5, F32)
        sends = []
        for i in range(n_tp * n_stage):
            tp, pp = i // n_stage, i % n_stage
            if (tp, pp) != (1, n_stage - 1):
                sends.append(rcopy(ltile, ltile, lsend.at[i], lrecv, tp, pp))
        for s in sends:
            s.start()
        for s in sends:
            s.wait_send()

    @pl.when(jnp.logical_not(owner))
    def _():
        wait_in(ltile, lrecv)

    lout = pltpu.make_async_copy(ltile, loss_out, tsem)
    lout.start()
    lout.wait()

    for slot in range(3):
        wait_in(sbuf.at[slot], ssem.at[slot])

    @pl.when(jnp.logical_not(first))
    def _():
        wait_in(sbuf.at[3], ssem.at[3])

    @pl.when(is_mid)
    def _():
        for slot in range(3):
            wait_in(obuf.at[slot], oesem.at[slot])

        @pl.when(jnp.logical_not(last))
        def _():
            wait_in(obuf.at[1], oosem.at[1])

        @pl.when(jnp.logical_not(first))
        def _():
            wait_in(obuf.at[3], oesem.at[3])
            wait_in(obuf.at[3], oosem.at[3])

    pltpu.make_async_copy(a_out, a_out, outsem.at[0]).wait()
    pltpu.make_async_copy(d_out, d_out, outsem.at[1]).wait()
    pltpu.make_async_copy(z_out, z_out, outsem.at[2]).wait()
    pltpu.make_async_copy(g_out, g_out, outsem.at[3]).wait()


def solution(mesh):
    n_stage = mesh.shape["pp"]
    n_tp = mesh.shape["tp"]
    assert n_tp == 4

    def device_program(x_loc, y_loc, w_in, w_out):
        n_micro, n_tok, d_model = x_loc.shape
        hidden = w_in.shape[3]
        dpc = d_model // NP
        inv_count = 1.0 / (n_micro * n_tok * d_model)
        rows = n_micro * n_tok
        save_d = jax.ShapeDtypeStruct((2, rows, d_model), BF)
        save_h = jax.ShapeDtypeStruct((2, rows, hidden), BF)
        dma = pltpu.SemaphoreType.DMA
        piece = (NP, n_tok, dpc)
        a_s, d_s, g_s, z_s, loss = pl.pallas_call(
            functools.partial(step_kernel, n_stage, n_tp, inv_count),
            out_shape=(save_d, save_d, save_h, save_h, jax.ShapeDtypeStruct((8, 128), F32)),
            in_specs=[pl.BlockSpec(memory_space=pl.ANY)] * 4,
            out_specs=[pl.BlockSpec(memory_space=pl.ANY)] * 5,
            scratch_shapes=[
                pltpu.VMEM((2, d_model, hidden), BF),
                pltpu.VMEM((2, hidden, d_model), BF),
                pltpu.VMEM((4, n_micro) + piece, BF),
                pltpu.VMEM((2, n_micro, n_tok, hidden), BF),
                pltpu.VMEM((2, n_micro, n_tok, hidden), BF),
                pltpu.VMEM((4, RING) + piece, BF),
                pltpu.VMEM((4, RING) + piece, BF),
                pltpu.VMEM((4,) + piece, BF),
                pltpu.VMEM((4,) + piece, BF),
                pltpu.VMEM((2,) + piece, F32),
                pltpu.VMEM((n_micro,) + piece, BF),
                pltpu.VMEM((8, dpc), F32),
                pltpu.VMEM((8, 128), F32),
                dma((2, n_micro, NP)), dma((2, RING, NP)), dma((4, RING, NP)), dma((4, RING, NP)),
                dma((4,)), dma((4,)), dma((4,)), dma((4,)), dma, dma((4,)), dma((n_tp * n_stage,)), dma,
            ],
            compiler_params=pltpu.CompilerParams(has_side_effects=True, vmem_limit_bytes=63 * 1024 * 1024),
            name="pipeline_step",
        )(x_loc, y_loc, w_in, w_out)
        grad_first = jnp.einsum("ktd,ktf->kdf", a_s, g_s, preferred_element_type=F32)[None]
        grad_second = jnp.einsum("ktf,ktd->kfd", z_s, d_s, preferred_element_type=F32)[None]
        return grad_first, grad_second, loss[0, :1]

    return jax.shard_map(
        device_program,
        mesh=mesh,
        in_specs=(P("dp", None, None), P("dp", None, None), P("pp", None, None, "tp"), P("pp", None, "tp", None)),
        out_specs=(P(("dp", "pp"), None, None, "tp"), P(("dp", "pp"), None, "tp", None), P("dp")),
        check_vma=False,
    )
```

```python
import functools
import math

import jax
import jax.numpy as jnp
from jax import lax
from jax.experimental import pallas as pl
from jax.experimental.pallas import tpu as pltpu
from jax.sharding import PartitionSpec as P

BF = jnp.bfloat16
F32 = jnp.float32
NP = 4
LB, LC = 1, 2
SR = 4
WCH = 8
GC = math.sqrt(2.0 / math.pi)
NT = (((1,), (1,)), ((), ()))
MESH = pl.DeviceIdType.MESH


def gelu_f(x):
    return x * (0.5 + 0.5 * jnp.tanh(GC * (x + 0.044715 * (x * x * x))))


def gelu_d(x):
    x2 = x * x
    th = jnp.tanh(GC * (x + 0.044715 * (x * x2)))
    return 0.5 + 0.5 * th + (0.5 * x) * (1.0 - th * th) * (GC + (3 * 0.044715 * GC) * x2)


def step_kernel(n_micro, inv_count, x_hbm, t_hbm, w1_hbm, w2_hbm,
                a_out, d_out, g_out, z_out, loss_out,
                w, act, ubuf, zbuf, pbuf, qbuf, sbuf, obuf, own, lacc, ltile,
                asem, psem, qsem, ssem, oesem, oosem, ldsem, tsem, outsem, lsend, lrecv,
                wrsem, wssem, wfsem, shsem, gosem):
    nh = n_micro // 2
    n_tok, dpc = act.shape[2:]
    hid = ubuf.shape[2]
    hb = hid // NP
    nd = 3 * n_micro
    rows_w = w.shape[2] // WCH
    stage = lax.axis_index("pp")
    z = lax.axis_index("tp")
    x = lax.axis_index("dp")
    y = stage // 2
    core = lax.rem(stage, 2)
    y0, y1 = y == 0, y == 1
    c0, c1 = core == 0, core == 1
    mirror = lax.rem(stage + 2, 4)
    is_mid = (z == 1) | (z == 2)
    is_end = jnp.logical_not(is_mid)
    partner = z + 1 - 2 * lax.rem(z, 2)
    other = 3 - z
    n_slots = n_micro + 15 * nh

    def rcopy(src, dst, s_sem, r_sem, tp, pp):
        return pltpu.make_async_remote_copy(src_ref=src, dst_ref=dst, send_sem=s_sem, recv_sem=r_sem,
                                            device_id={"tp": tp, "pp": pp}, device_id_type=MESH)

    def wait_in(ref, sem):
        pltpu.make_async_copy(ref, ref, sem).wait()

    def decode(n):
        nn = jnp.maximum(n - n_micro, 0)
        r0 = n < n_micro
        rho = jnp.where(r0, 0, 1 + nn // nh)
        j = jnp.where(r0, n // 2, lax.rem(nn, nh))
        ext = r0 & (lax.rem(n + 2, 2) == 1)
        m = jnp.where(r0, j + nh * lax.rem(n + 2, 2), nh * y + j)
        fwd = rho < 8
        l = jnp.where(fwd, rho, 15 - rho)
        ok = (n >= 0) & (n < n_slots) & (lax.rem(l // 2, 2) == core)
        ok = ok & (y0 | ((rho > 0) & (rho < 15)))
        return dict(n=n, rho=rho, j=j, ext=ext, m=m, fwd=fwd, l=l, ok=ok, ar=ok & (rho < 15))

    def index_of(l, m, j, yy):
        home = (l // 4) == yy
        return jnp.where(home, lax.rem(l, 2) * n_micro + m, 2 * n_micro + lax.rem(l, 2) * nh + j)

    def p_slot(e):
        return jnp.where(e["ext"], nh + e["j"], e["j"])

    def q_slot(e):
        return jnp.where(e["ext"], 2 * nh + e["j"], lax.rem(e["rho"], 2) * nh + e["j"])

    def dest(e):
        l, m, j, fwd = e["l"], e["m"], e["j"], e["fwd"]
        last = fwd & (l == 7)
        dl = jnp.where(fwd, jnp.where(last, 7, l + 1), l - 1)
        dy = jnp.where(e["ext"], 1, jnp.where(jnp.logical_not(fwd) & (l == 1), 0, y))
        dc = lax.rem(dl // 2, 2)
        grad = last | jnp.logical_not(fwd)
        di = index_of(dl, m, j, dy) + jnp.where(grad, nd, 0)
        return last, di, 2 * dy + dc, (dy == y) & (dc == core)

    loads = []
    for k in range(2):
        loads.append(pltpu.make_async_copy(w1_hbm.at[0, k], w.at[2 * y + k, 0], ldsem.at[k]))
        loads.append(pltpu.make_async_copy(w2_hbm.at[0, k], w.at[2 * y + k, 1], ldsem.at[2 + k]))
    for ld in loads:
        ld.start()

    @pl.when(y0 & c0)
    def _():
        @pl.loop(0, n_micro)
        def _(m):
            for c in range(NP):
                pltpu.make_async_copy(x_hbm.at[m, :, pl.ds(c * dpc, dpc)], act.at[m, c], asem.at[m, c]).start()

    lacc[...] = jnp.zeros_like(lacc)
    t_base = nd + index_of(7, nh * y, 0, y)

    @pl.when(c1 & is_mid)
    def _():
        @pl.loop(0, nh)
        def _(j):
            for c in range(NP):
                pltpu.make_async_copy(t_hbm.at[nh * y + j, :, pl.ds(c * dpc, dpc)], act.at[t_base + j, c], tsem).start()
        wait_in(act.at[pl.ds(t_base, nh)], tsem)

    for ld in loads:
        ld.wait()

    def send_weights(k):
        for i in range(WCH):
            half, g = i // (WCH // 2), lax.rem(2 * i, WCH) + x
            src = w.at[2 * y + k, half, pl.ds(g * rows_w, rows_w)]
            rcopy(src, src, wssem, wrsem.at[k, half, g], z, mirror).start()

    pl.when(jnp.logical_not(y0))(functools.partial(send_weights, 0))
    pl.when(c0 | y1)(functools.partial(send_weights, 1))

    @pl.when(y0 & c1)
    def _():
        pl.semaphore_wait(gosem, 1)
        send_weights(0)
        send_weights(1)

    n_chunk = jnp.where(y1 & c0, WCH, 2 * WCH)
    relay0 = jnp.where(y0, jnp.where(c0, 2, 26), jnp.where(c0, 0, 8))

    def relay(i):
        k = jnp.where(y1 & c0, 1, i // WCH)
        i = lax.rem(i, WCH)
        half = i // (WCH // 2)
        g = lax.rem(2 * i, WCH) + x
        ref = w.at[2 * (1 - y) + k, half, pl.ds(pl.multiple_of(g * rows_w, rows_w), rows_w)]
        wait_in(ref, wrsem.at[k, half, g])
        pltpu.make_async_remote_copy(src_ref=ref, dst_ref=ref, send_sem=wfsem, recv_sem=wrsem.at[k, half, g],
                                     device_id={"dp": 1 - x}, device_id_type=MESH).start()

    def wait_weights(k):
        for i in range(WCH):
            half, g = i // (WCH // 2), lax.rem(2 * i, WCH) + (1 - x)
            ref = w.at[2 * (1 - y) + k, half, pl.ds(pl.multiple_of(g * rows_w, rows_w), rows_w)]
            wait_in(ref, wrsem.at[k, half, g])

    def load_full(ai):
        return jnp.concatenate([act[ai, c] for c in range(NP)], axis=1)

    def put_act(ai, k, m, dst, sem):
        for c in range(NP):
            pltpu.make_async_copy(act.at[ai, c], dst.at[k, pl.ds(pl.multiple_of(m * n_tok, n_tok), n_tok), pl.ds(c * dpc, dpc)], sem).start()

    def put_hid(src, k, m, dst, sem):
        pltpu.make_async_copy(src, dst.at[k, pl.ds(pl.multiple_of(m * n_tok, n_tok), n_tok)], sem).start()

    def ship(ai, hi):
        rcopy(act.at[ai], act.at[hi], shsem, asem.at[hi, 0], z, mirror).start()

    def up_fwd(ai, wi, zi):
        a = load_full(ai)
        for n in range(NP):
            cs = pl.ds(n * hb, hb)
            u = jnp.dot(a, w[wi, 0, :, cs], preferred_element_type=F32).astype(BF)
            ubuf[ai, :, cs] = u
            zbuf[zi, :, cs] = gelu_f(u.astype(F32)).astype(BF)

    def up_bwd(ai, wi):
        d = load_full(nd + ai)
        for n in range(NP):
            cs = pl.ds(n * hb, hb)
            up = lax.dot_general(d, w[wi, 1, cs, :], NT, preferred_element_type=F32)
            ubuf[ai, :, cs] = (gelu_d(ubuf[ai, :, cs].astype(F32)) * up).astype(BF)

    def emit_piece(e, c, part):
        @pl.when(is_end)
        def _():
            s, r = lax.rem(e["n"], SR), p_slot(e)
            sbuf[s, c] = part.astype(BF)
            rcopy(sbuf.at[s, c], pbuf.at[r, c], ssem.at[s], psem.at[r, c], partner, stage).start()

        @pl.when(is_mid)
        def _():
            own[lax.rem(e["n"], LB + 1), c] = part

    def do_a(e):
        l, m, j, fwd = e["l"], e["m"], e["j"], e["fwd"]
        k = lax.rem(l, 2)
        home = (l // 4) == y
        wi = 2 * (l // 4) + k
        ai = index_of(l, m, j, y)
        hi = k * n_micro + m
        odd = k == 1

        @pl.when(fwd)
        def _():
            @pl.when(is_end | (k == 0) | ((l == 1) & y1))
            def _():
                for c in range(NP):
                    wait_in(act.at[ai, c], asem.at[ai, c])

            @pl.when(jnp.logical_not(home))
            def _():
                ship(ai, hi)
                pl.when(j == 0)(functools.partial(wait_weights, k))

            zi = jnp.where(home, hi, 2 * n_micro)
            up_fwd(ai, wi, zi)

            @pl.when(home)
            def _():
                put_act(ai, k, m, a_out, outsem.at[0])
                put_hid(zbuf.at[zi], k, m, z_out, outsem.at[2])

            zz = zbuf[zi]
            for c in range(NP):
                emit_piece(e, c, jnp.dot(zz, w[wi, 1, :, pl.ds(c * dpc, dpc)], preferred_element_type=F32))

        @pl.when(jnp.logical_not(fwd))
        def _():
            @pl.when(is_end | (odd & (l < 7)))
            def _():
                for c in range(NP):
                    wait_in(act.at[nd + ai, c], asem.at[nd + ai, c])

            pl.when(jnp.logical_not(home))(functools.partial(ship, nd + ai, nd + hi))
            up_bwd(ai, wi)

            @pl.when(home)
            def _():
                put_act(nd + ai, k, m, d_out, outsem.at[1])
                put_hid(ubuf.at[ai], k, m, g_out, outsem.at[3])

            @pl.when(e["ar"])
            def _():
                gg = ubuf[ai]
                for c in range(NP):
                    emit_piece(e, c, lax.dot_general(gg, w[wi, 0, pl.ds(c * dpc, dpc), :], NT, preferred_element_type=F32))

    def do_b(e):
        s, r, qr = lax.rem(e["n"], SR), p_slot(e), q_slot(e)
        so = lax.rem(e["n"], LB + 1)
        for c in range(NP):
            wait_in(pbuf.at[r, c], psem.at[r, c])
            sbuf[s, c] = (own[so, c] + pbuf[r, c].astype(F32)).astype(BF)
            rcopy(sbuf.at[s, c], qbuf.at[qr, c], ssem.at[s], qsem.at[qr, c], other, stage).start()

    def do_c(e):
        s, qr = lax.rem(e["n"], SR), q_slot(e)
        ai = index_of(e["l"], e["m"], e["j"], y) + jnp.where(e["fwd"], 0, nd)
        last, di, ds, local = dest(e)
        for c in range(NP):
            wait_in(qbuf.at[qr, c], qsem.at[qr, c])
            h = act[ai, c].astype(F32) + (sbuf[s, c].astype(F32) + qbuf[qr, c].astype(F32))
            h = h.astype(BF)

            @pl.when(last)
            def _():
                err = h.astype(F32) - act[di, c].astype(F32)
                lacc[...] += jnp.sum((err * err).reshape(n_tok // 8, 8, dpc), axis=0)
                dy = (err * inv_count).astype(BF)
                obuf[s, c] = dy
                act[di, c] = dy

            @pl.when(jnp.logical_not(last))
            def _():
                obuf[s, c] = h

                @pl.when(local)
                def _():
                    act[di, c] = h

            @pl.when(jnp.logical_not(local))
            def _():
                rcopy(obuf.at[s, c], act.at[di, c], oosem.at[s], asem.at[di, c], z, ds).start()

            rcopy(obuf.at[s, c], act.at[di, c], oesem.at[s], asem.at[di, c], partner, ds).start()

    redo0 = jnp.where(y0, jnp.where(c0, n_slots - nh, n_slots - 2 * nh), jnp.where(c0, n_slots - 4 * nh, n_slots - 6 * nh))

    def redo(i):
        k = 1 - i // nh
        m = nh * (1 - y) + lax.rem(i, nh)
        hi = k * n_micro + m
        wi = 2 * y + k
        layer0 = y0 & c0 & (k == 0)

        @pl.when(jnp.logical_not(layer0))
        def _():
            wait_in(act.at[hi], asem.at[hi, 0])
            wait_in(act.at[nd + hi], asem.at[nd + hi, 0])
            put_act(hi, k, m, a_out, outsem.at[0])
            up_fwd(hi, wi, hi)
            put_hid(zbuf.at[hi], k, m, z_out, outsem.at[2])

        @pl.when(layer0)
        def _():
            for c in range(NP):
                wait_in(act.at[nd + hi, c], asem.at[nd + hi, c])

        put_act(nd + hi, k, m, d_out, outsem.at[1])
        up_bwd(hi, wi)
        put_hid(ubuf.at[hi], k, m, g_out, outsem.at[3])

    def slot(n, carry):
        e = decode(n)
        old = decode(n - SR)
        eb, ebo = decode(n - LB), decode(n - LB - SR)
        ec, eco = decode(n - LC), decode(n - LC - SR)

        @pl.when((is_end & old["ar"]) | (is_mid & ebo["ar"]))
        def _():
            s = lax.rem(n + SR - jnp.where(is_end, 0, LB), SR)
            wait_in(sbuf.at[s], ssem.at[s])

        @pl.when(is_mid & eco["ar"])
        def _():
            s = lax.rem(n + SR - LC, SR)
            wait_in(obuf.at[s], oesem.at[s])
            local = dest(eco)[3]
            pl.when(jnp.logical_not(local))(lambda: wait_in(obuf.at[s], oosem.at[s]))

        pl.when(e["ok"])(functools.partial(do_a, e))
        pl.when(is_mid & eb["ar"])(functools.partial(do_b, eb))
        pl.when(is_mid & ec["ar"])(functools.partial(do_c, ec))
        ri = n - relay0
        pl.when((ri >= 0) & (ri < n_chunk))(functools.partial(relay, ri))

        @pl.when(y0 & c0 & (n == 8))
        def _():
            wait_in(w.at[1, 0], wssem)
            pl.semaphore_signal(gosem, 1, device_id={"pp": 1}, device_id_type=MESH)

        di = n - redo0
        pl.when((di >= 0) & (di < 2 * nh))(functools.partial(redo, di))
        return carry

    lax.fori_loop(0, n_slots + LC + SR + 2, slot, 0)

    owner = (z == 1) & c1

    @pl.when(owner)
    def _():
        ltile[y] = jnp.full(ltile.shape[1:], jnp.sum(lacc[...]) * inv_count * 0.5, F32)
        for i in range(16):
            tp, pp = i // 4, i % 4

            @pl.when((tp != 1) | (pp != stage))
            def _():
                rcopy(ltile.at[y], ltile.at[y], lsend.at[i], lrecv.at[y], tp, pp).start()
        for i in range(16):
            tp, pp = i // 4, i % 4

            @pl.when((tp != 1) | (pp != stage))
            def _():
                wait_in(ltile.at[y], lsend.at[i])

    for yy in range(2):
        @pl.when(jnp.logical_not(owner & (y == yy)))
        def _():
            wait_in(ltile.at[yy], lrecv.at[yy])

    ltile[0] = ltile[0] + ltile[1]
    lout = pltpu.make_async_copy(ltile.at[0], loss_out, tsem)
    lout.start()
    lout.wait()

    for full, sem in ((jnp.logical_not(y0 & c0), wssem), (jnp.logical_not(y1 & c0), wfsem)):
        pl.when(full)(functools.partial(wait_in, w.at[0], sem))
    pl.when(y1 & c0)(functools.partial(wait_in, w.at[0, 0], wfsem))
    half_ship = y1 & c0
    pl.when(half_ship)(functools.partial(wait_in, act.at[pl.ds(0, n_micro)], shsem))
    pl.when(jnp.logical_not(half_ship))(functools.partial(wait_in, act.at[pl.ds(0, 2 * n_micro)], shsem))
    pltpu.make_async_copy(a_out, a_out, outsem.at[0]).wait()
    pltpu.make_async_copy(d_out, d_out, outsem.at[1]).wait()
    pltpu.make_async_copy(z_out, z_out, outsem.at[2]).wait()
    pltpu.make_async_copy(g_out, g_out, outsem.at[3]).wait()


def solution(mesh):
    assert (mesh.shape["tp"], mesh.shape["pp"], mesh.shape["dp"]) == (4, 4, 2)

    def device_program(x_loc, y_loc, w_in, w_out):
        n_micro, n_tok, d_model = x_loc.shape
        hidden = w_in.shape[3]
        assert d_model == hidden and n_micro % 2 == 0
        dpc = d_model // NP
        nh = n_micro // 2
        inv_count = 1.0 / (n_micro * n_tok * d_model)
        rows = n_micro * n_tok
        save_d = jax.ShapeDtypeStruct((2, rows, d_model), BF)
        save_h = jax.ShapeDtypeStruct((2, rows, hidden), BF)
        dma = pltpu.SemaphoreType.DMA
        piece = (NP, n_tok, dpc)
        a_s, d_s, g_s, z_s, loss = pl.pallas_call(
            functools.partial(step_kernel, n_micro, inv_count),
            out_shape=(save_d, save_d, save_h, save_h, jax.ShapeDtypeStruct((8, 128), F32)),
            in_specs=[pl.BlockSpec(memory_space=pl.ANY)] * 4,
            out_specs=[pl.BlockSpec(memory_space=pl.ANY)] * 5,
            scratch_shapes=[
                pltpu.VMEM((4, 2, d_model, hidden), BF),
                pltpu.VMEM((6 * n_micro,) + piece, BF),
                pltpu.VMEM((3 * n_micro, n_tok, hidden), BF),
                pltpu.VMEM((2 * n_micro + 1, n_tok, hidden), BF),
                pltpu.VMEM((2 * nh,) + piece, BF),
                pltpu.VMEM((3 * nh,) + piece, BF),
                pltpu.VMEM((SR,) + piece, BF),
                pltpu.VMEM((SR,) + piece, BF),
                pltpu.VMEM((LB + 1,) + piece, F32),
                pltpu.VMEM((8, dpc), F32),
                pltpu.VMEM((2, 8, 128), F32),
                dma((6 * n_micro, NP)), dma((2 * nh, NP)), dma((3 * nh, NP)),
                dma((SR,)), dma((SR,)), dma((SR,)), dma((4,)), dma, dma((4,)), dma((16,)), dma((2,)),
                dma((2, 2, WCH)), dma, dma, dma, pltpu.SemaphoreType.REGULAR,
            ],
            compiler_params=pltpu.CompilerParams(has_side_effects=True, vmem_limit_bytes=67043328),
            name="pipeline_step",
        )(x_loc, y_loc, w_in, w_out)
        grad_first = jnp.einsum("ktd,ktf->kdf", a_s, g_s, preferred_element_type=F32)[None]
        grad_second = jnp.einsum("ktf,ktd->kfd", z_s, d_s, preferred_element_type=F32)[None]
        return grad_first, grad_second, loss[0, :1]

    return jax.shard_map(
        device_program,
        mesh=mesh,
        in_specs=(P("dp", None, None), P("dp", None, None), P("pp", None, None, "tp"), P("pp", None, "tp", None)),
        out_specs=(P(("dp", "pp"), None, None, "tp"), P(("dp", "pp"), None, "tp", None), P("dp")),
        check_vma=False,
    )
```

```python
import functools
import math

import jax
import jax.numpy as jnp
from jax import lax
from jax.experimental import pallas as pl
from jax.experimental.pallas import tpu as pltpu
from jax.sharding import PartitionSpec as P

BF = jnp.bfloat16
F32 = jnp.float32
NP = 2
FB, BB, EF, EB = 4, 8, 4, 8
LB, LC = 1, 3
SR = 4
WCH = 8
GC = math.sqrt(2.0 / math.pi)
NT = (((1,), (1,)), ((), ()))
MESH = pl.DeviceIdType.MESH


def gelu_f(x):
    return x * (0.5 + 0.5 * jnp.tanh(GC * (x + 0.044715 * (x * x * x))))


def gelu_d(x):
    x2 = x * x
    th = jnp.tanh(GC * (x + 0.044715 * (x * x2)))
    return 0.5 + 0.5 * th + (0.5 * x) * (1.0 - th * th) * (GC + (3 * 0.044715 * GC) * x2)


def step_kernel(n_micro, inv_count, x_hbm, t_hbm, w1_hbm, w2_hbm,
                a_out, d_out, g_out, z_out, loss_out,
                w, act, ubuf, zbuf, pbuf, qbuf, sbuf, obuf, own, lacc, ltile,
                asem, psem, qsem, ssem, oesem, oosem, ldsem, tsem, outsem, lsend, lrecv,
                wrsem, wssem, wfsem, shsem, pxsem, gosem):
    nh = n_micro // 2
    n_tok, dpc = act.shape[2:]
    hid = ubuf.shape[2]
    nd = 3 * n_micro
    rows_w = w.shape[2] // WCH
    stage = lax.axis_index("pp")
    z = lax.axis_index("tp")
    x = lax.axis_index("dp")
    y = stage // 2
    core = lax.rem(stage, 2)
    y0, y1 = y == 0, y == 1
    c0, c1 = core == 0, core == 1
    mirror = lax.rem(stage + 2, 4)
    is_mid = (z == 1) | (z == 2)
    is_end = jnp.logical_not(is_mid)
    partner = z + 1 - 2 * lax.rem(z, 2)
    other = 3 - z
    n_slots = n_micro + 15 * nh

    def rcopy(src, dst, s_sem, r_sem, tp, pp):
        return pltpu.make_async_remote_copy(src_ref=src, dst_ref=dst, send_sem=s_sem, recv_sem=r_sem,
                                            device_id={"tp": tp, "pp": pp}, device_id_type=MESH)

    def wait_in(ref, sem):
        pltpu.make_async_copy(ref, ref, sem).wait()

    def decode(n):
        nn = jnp.maximum(n - n_micro, 0)
        r0 = n < n_micro
        rho = jnp.where(r0, 0, 1 + nn // nh)
        ext = n < nh
        j = jnp.where(r0, jnp.where(ext, n, n - nh), lax.rem(nn, nh))
        m = jnp.where(r0, jnp.where(ext, n + nh, n - nh), nh * y + j)
        fwd = rho < 8
        l = jnp.where(fwd, rho, 15 - rho)
        ok = (n >= 0) & (n < n_slots) & (lax.rem(l // 2, 2) == core)
        ok = ok & (y0 | ((rho > 0) & (rho < 15)))
        return dict(n=n, rho=rho, j=j, ext=ext, m=m, fwd=fwd, l=l, ok=ok, ar=ok & (rho < 15))

    def index_of(l, m, j, yy):
        home = (l // 4) == yy
        return jnp.where(home, lax.rem(l, 2) * n_micro + m, 2 * n_micro + lax.rem(l, 2) * nh + j)

    def p_slot(e):
        return jnp.where(e["ext"], nh + e["j"], e["j"])

    def q_slot(e):
        return jnp.where(e["ext"], 2 * nh + e["j"], lax.rem(e["rho"], 2) * nh + e["j"])

    def dest(e):
        l, m, j, fwd = e["l"], e["m"], e["j"], e["fwd"]
        last = fwd & (l == 7)
        dl = jnp.where(fwd, jnp.where(last, 7, l + 1), l - 1)
        dy = jnp.where(e["ext"], 1, jnp.where(jnp.logical_not(fwd) & (l == 1), 0, y))
        dc = lax.rem(dl // 2, 2)
        grad = last | jnp.logical_not(fwd)
        di = index_of(dl, m, j, dy) + jnp.where(grad, nd, 0)
        return last, di, 2 * dy + dc, (dy == y) & (dc == core)

    loads = []
    for k in range(2):
        loads.append(pltpu.make_async_copy(w1_hbm.at[0, k], w.at[2 * y + k, 0], ldsem.at[k]))
        loads.append(pltpu.make_async_copy(w2_hbm.at[0, k], w.at[2 * y + k, 1], ldsem.at[2 + k]))
    for ld in loads:
        ld.start()

    @pl.when(y0 & c0)
    def _():
        @pl.loop(0, n_micro)
        def _(m):
            for c in range(NP):
                pltpu.make_async_copy(x_hbm.at[m, :, pl.ds(c * dpc, dpc)], act.at[m, c], asem.at[m, c]).start()

    lacc[...] = jnp.zeros_like(lacc)
    t_base = nd + index_of(7, nh * y, 0, y)

    @pl.when(c1 & is_mid)
    def _():
        @pl.loop(0, nh)
        def _(j):
            for c in range(NP):
                pltpu.make_async_copy(t_hbm.at[nh * y + j, :, pl.ds(c * dpc, dpc)], act.at[t_base + j, c], tsem).start()
        wait_in(act.at[pl.ds(t_base, nh)], tsem)

    for ld in loads:
        ld.wait()

    def send_weights(k):
        for i in range(WCH):
            half, g = i // (WCH // 2), lax.rem(2 * i, WCH) + x
            src = w.at[2 * y + k, half, pl.ds(g * rows_w, rows_w)]
            rcopy(src, src, wssem, wrsem.at[k, half, g], z, mirror).start()

    pl.when(jnp.logical_not(y0))(functools.partial(send_weights, 0))
    pl.when(c0 | y1)(functools.partial(send_weights, 1))

    @pl.when(y0 & c1)
    def _():
        pl.semaphore_wait(gosem, 1)
        send_weights(0)
        send_weights(1)

    n_chunk = jnp.where(y1 & c0, WCH, 2 * WCH)
    relay0 = jnp.where(y0, jnp.where(c0, 2, 26), jnp.where(c0, 0, 8))

    def relayed(n):
        late = jnp.where(n < 19, jnp.clip(n - relay0, 0, WCH), jnp.where(n < 24, n - 11, 2 * WCH))
        slow = jnp.clip((n - 4) // 2, 0, n_chunk)
        return jnp.where(y1 & c1 & (n > 8), late, jnp.where(y0 & c0, slow, jnp.clip(n - relay0, 0, n_chunk)))

    def relay(i):
        k = jnp.where(y1 & c0, 1, i // WCH)
        i = lax.rem(i, WCH)
        half = i // (WCH // 2)
        g = lax.rem(2 * i, WCH) + x
        ref = w.at[2 * (1 - y) + k, half, pl.ds(pl.multiple_of(g * rows_w, rows_w), rows_w)]
        wait_in(ref, wrsem.at[k, half, g])
        pltpu.make_async_remote_copy(src_ref=ref, dst_ref=ref, send_sem=wfsem, recv_sem=wrsem.at[k, half, g],
                                     device_id={"dp": 1 - x}, device_id_type=MESH).start()

    def wait_weights(k):
        for i in range(WCH):
            half, g = i // (WCH // 2), lax.rem(2 * i, WCH) + (1 - x)
            ref = w.at[2 * (1 - y) + k, half, pl.ds(pl.multiple_of(g * rows_w, rows_w), rows_w)]
            wait_in(ref, wrsem.at[k, half, g])

    def load_full(ai):
        return jnp.concatenate([act[ai, c] for c in range(NP)], axis=1)

    def put_act(ai, k, m, dst, sem):
        for c in range(NP):
            pltpu.make_async_copy(act.at[ai, c], dst.at[k, pl.ds(pl.multiple_of(m * n_tok, n_tok), n_tok), pl.ds(c * dpc, dpc)], sem).start()

    def put_hid(src, k, m, dst, sem):
        pltpu.make_async_copy(src, dst.at[k, pl.ds(pl.multiple_of(m * n_tok, n_tok), n_tok)], sem).start()

    def ship(ai, hi):
        rcopy(act.at[ai], act.at[hi], shsem, asem.at[hi, 0], z, mirror).start()

    def up_fwd(ai, wi, zi):
        a = load_full(ai)
        hb = hid // FB
        for n in range(FB):
            cs = pl.ds(n * hb, hb)
            u = jnp.dot(a, w[wi, 0, :, cs], preferred_element_type=F32).astype(BF)
            ubuf[ai, :, cs] = u
            zbuf[zi, :, cs] = gelu_f(u.astype(F32)).astype(BF)

    def up_bwd(ai, wi):
        d = load_full(nd + ai)
        hb = hid // BB
        for n in range(BB):
            cs = pl.ds(n * hb, hb)
            up = lax.dot_general(d, w[wi, 1, cs, :], NT, preferred_element_type=F32)
            ubuf[ai, :, cs] = (gelu_d(ubuf[ai, :, cs].astype(F32)) * up).astype(BF)

    def emit(e, nb, product):
        bw, per = dpc * NP // nb, nb // NP
        for c in range(NP):
            parts = [product(pl.ds((c * per + i) * bw, bw)) for i in range(per)]

            @pl.when(is_end)
            def _():
                s, r = lax.rem(e["n"], SR), p_slot(e)
                for i, part in enumerate(parts):
                    sbuf[s, c, :, pl.ds(i * bw, bw)] = part.astype(BF)
                rcopy(sbuf.at[s, c], pbuf.at[r, c], ssem.at[s], psem.at[r, c], partner, stage).start()

            @pl.when(is_mid)
            def _():
                for i, part in enumerate(parts):
                    own[lax.rem(e["n"], LB + 1), c, :, pl.ds(i * bw, bw)] = part

    def do_a(e):
        l, m, j, fwd = e["l"], e["m"], e["j"], e["fwd"]
        k = lax.rem(l, 2)
        home = (l // 4) == y
        wi = 2 * (l // 4) + k
        ai = index_of(l, m, j, y)
        hi = k * n_micro + m
        odd = k == 1

        @pl.when(fwd)
        def _():
            @pl.when(is_end | (k == 0) | ((l == 1) & y1))
            def _():
                for c in range(NP):
                    wait_in(act.at[ai, c], asem.at[ai, c])

                    @pl.when(is_mid & (l == 1))
                    def _():
                        rcopy(act.at[ai, c], act.at[ai, c], pxsem, asem.at[ai, c], partner, stage).start()

            @pl.when(jnp.logical_not(home))
            def _():
                ship(ai, hi)
                pl.when(j == 0)(functools.partial(wait_weights, k))

            zi = jnp.where(home, hi, 2 * n_micro)
            up_fwd(ai, wi, zi)

            @pl.when(home)
            def _():
                put_act(ai, k, m, a_out, outsem.at[0])
                put_hid(zbuf.at[zi], k, m, z_out, outsem.at[2])

            zz = zbuf[zi]
            emit(e, EF, lambda cs: jnp.dot(zz, w[wi, 1, :, cs], preferred_element_type=F32))

        @pl.when(jnp.logical_not(fwd))
        def _():
            @pl.when(is_end | (odd & (l < 7)))
            def _():
                for c in range(NP):
                    wait_in(act.at[nd + ai, c], asem.at[nd + ai, c])

            pl.when(jnp.logical_not(home))(functools.partial(ship, nd + ai, nd + hi))
            up_bwd(ai, wi)

            @pl.when(home)
            def _():
                put_act(nd + ai, k, m, d_out, outsem.at[1])
                put_hid(ubuf.at[ai], k, m, g_out, outsem.at[3])

            @pl.when(e["ar"])
            def _():
                gg = ubuf[ai]
                emit(e, EB, lambda cs: lax.dot_general(gg, w[wi, 0, cs, :], NT, preferred_element_type=F32))

    def do_b(e):
        s, r, qr = lax.rem(e["n"], SR), p_slot(e), q_slot(e)
        so = lax.rem(e["n"], LB + 1)
        for c in range(NP):
            wait_in(pbuf.at[r, c], psem.at[r, c])
            sbuf[s, c] = (own[so, c] + pbuf[r, c].astype(F32)).astype(BF)
            rcopy(sbuf.at[s, c], qbuf.at[qr, c], ssem.at[s], qsem.at[qr, c], other, stage).start()

    def do_c(e):
        s, qr = lax.rem(e["n"], SR), q_slot(e)
        ai = index_of(e["l"], e["m"], e["j"], y) + jnp.where(e["fwd"], 0, nd)
        last, di, ds, local = dest(e)
        for c in range(NP):
            wait_in(qbuf.at[qr, c], qsem.at[qr, c])
            h = act[ai, c].astype(F32) + (sbuf[s, c].astype(F32) + qbuf[qr, c].astype(F32))
            h = h.astype(BF)

            @pl.when(last)
            def _():
                err = h.astype(F32) - act[di, c].astype(F32)
                lacc[...] += jnp.sum((err * err).reshape(n_tok // 8, 8, dpc), axis=0)
                dy = (err * inv_count).astype(BF)
                obuf[s, c] = dy
                act[di, c] = dy

            @pl.when(jnp.logical_not(last))
            def _():
                obuf[s, c] = h

                @pl.when(local)
                def _():
                    act[di, c] = h

            @pl.when(jnp.logical_not(local))
            def _():
                rcopy(obuf.at[s, c], act.at[di, c], oosem.at[s], asem.at[di, c], z, ds).start()

            @pl.when(jnp.logical_not(e["ext"]))
            def _():
                rcopy(obuf.at[s, c], act.at[di, c], oesem.at[s], asem.at[di, c], partner, ds).start()

    redo_b0 = jnp.where(y0, jnp.where(c0, n_slots - nh, n_slots - 2 * nh), jnp.where(c0, n_slots - 4 * nh, n_slots - 6 * nh))
    redo_f0 = jnp.where(y0, jnp.where(c0, n_slots - 9 * nh, n_slots - 6 * nh), jnp.where(c0, n_slots - 8 * nh, n_slots - 6 * nh))
    n_redo_f = jnp.where(y0 & c0, nh, 2 * nh)

    def redo_at(i):
        k = 1 - i // nh
        m = nh * (1 - y) + lax.rem(i, nh)
        return k, m, k * n_micro + m, 2 * y + k

    def redo_f(i):
        k, m, hi, wi = redo_at(i)
        wait_in(act.at[hi], asem.at[hi, 0])
        put_act(hi, k, m, a_out, outsem.at[0])
        up_fwd(hi, wi, hi)
        put_hid(zbuf.at[hi], k, m, z_out, outsem.at[2])

    def redo_b(i):
        k, m, hi, wi = redo_at(i)
        layer0 = y0 & c0 & (k == 0)

        @pl.when(jnp.logical_not(layer0))
        def _():
            wait_in(act.at[nd + hi], asem.at[nd + hi, 0])

        @pl.when(layer0)
        def _():
            for c in range(NP):
                wait_in(act.at[nd + hi, c], asem.at[nd + hi, c])

        put_act(nd + hi, k, m, d_out, outsem.at[1])
        up_bwd(hi, wi)
        put_hid(ubuf.at[hi], k, m, g_out, outsem.at[3])

    def slot(n, carry):
        e = decode(n)
        old = decode(n - SR)
        eb, ebo = decode(n - LB), decode(n - LB - SR)
        ec, eco = decode(n - LC), decode(n - LC - SR)

        @pl.when((is_end & old["ar"]) | (is_mid & ebo["ar"]))
        def _():
            s = lax.rem(n + SR - jnp.where(is_end, 0, LB), SR)
            wait_in(sbuf.at[s], ssem.at[s])

        @pl.when(is_mid & eco["ar"])
        def _():
            s = lax.rem(n + SR - LC, SR)
            pl.when(jnp.logical_not(eco["ext"]))(lambda: wait_in(obuf.at[s], oesem.at[s]))
            local = dest(eco)[3]
            pl.when(jnp.logical_not(local))(lambda: wait_in(obuf.at[s], oosem.at[s]))

        @pl.loop(relayed(n), relayed(n + 1))
        def _(i):
            relay(i)

        pl.when(e["ok"])(functools.partial(do_a, e))
        pl.when(is_mid & ec["ar"])(functools.partial(do_c, ec))
        pl.when(is_mid & eb["ar"])(functools.partial(do_b, eb))

        @pl.when(y0 & c0 & (n == 6))
        def _():
            wait_in(w.at[1, 0], wssem)
            pl.semaphore_signal(gosem, 1, device_id={"pp": 1}, device_id_type=MESH)

        fi = n - redo_f0
        pl.when((fi >= 0) & (fi < n_redo_f))(functools.partial(redo_f, fi))
        bi = n - redo_b0
        pl.when((bi >= 0) & (bi < 2 * nh))(functools.partial(redo_b, bi))
        return carry

    lax.fori_loop(0, n_slots + LC + SR + 2, slot, 0)

    owner = (z == 1) & c1

    @pl.when(owner)
    def _():
        ltile[y] = jnp.full(ltile.shape[1:], jnp.sum(lacc[...]) * inv_count * 0.5, F32)
        for i in range(16):
            tp, pp = i // 4, i % 4

            @pl.when((tp != 1) | (pp != stage))
            def _():
                rcopy(ltile.at[y], ltile.at[y], lsend.at[i], lrecv.at[y], tp, pp).start()
        for i in range(16):
            tp, pp = i // 4, i % 4

            @pl.when((tp != 1) | (pp != stage))
            def _():
                wait_in(ltile.at[y], lsend.at[i])

    for yy in range(2):
        @pl.when(jnp.logical_not(owner & (y == yy)))
        def _():
            wait_in(ltile.at[yy], lrecv.at[yy])

    ltile[0] = ltile[0] + ltile[1]
    lout = pltpu.make_async_copy(ltile.at[0], loss_out, tsem)
    lout.start()
    lout.wait()

    for full, sem in ((jnp.logical_not(y0 & c0), wssem), (jnp.logical_not(y1 & c0), wfsem)):
        pl.when(full)(functools.partial(wait_in, w.at[0], sem))
    pl.when(y1 & c0)(functools.partial(wait_in, w.at[0, 0], wfsem))
    pl.when(y1 & c0 & is_mid)(functools.partial(wait_in, act.at[pl.ds(0, nh)], pxsem))
    half_ship = y1 & c0
    pl.when(half_ship)(functools.partial(wait_in, act.at[pl.ds(0, n_micro)], shsem))
    pl.when(jnp.logical_not(half_ship))(functools.partial(wait_in, act.at[pl.ds(0, 2 * n_micro)], shsem))
    pltpu.make_async_copy(a_out, a_out, outsem.at[0]).wait()
    pltpu.make_async_copy(d_out, d_out, outsem.at[1]).wait()
    pltpu.make_async_copy(z_out, z_out, outsem.at[2]).wait()
    pltpu.make_async_copy(g_out, g_out, outsem.at[3]).wait()


def solution(mesh):
    assert (mesh.shape["tp"], mesh.shape["pp"], mesh.shape["dp"]) == (4, 4, 2)

    def device_program(x_loc, y_loc, w_in, w_out):
        n_micro, n_tok, d_model = x_loc.shape
        hidden = w_in.shape[3]
        assert d_model == hidden and n_micro % 2 == 0
        dpc = d_model // NP
        nh = n_micro // 2
        inv_count = 1.0 / (n_micro * n_tok * d_model)
        rows = n_micro * n_tok
        save_d = jax.ShapeDtypeStruct((2, rows, d_model), BF)
        save_h = jax.ShapeDtypeStruct((2, rows, hidden), BF)
        dma = pltpu.SemaphoreType.DMA
        piece = (NP, n_tok, dpc)
        a_s, d_s, g_s, z_s, loss = pl.pallas_call(
            functools.partial(step_kernel, n_micro, inv_count),
            out_shape=(save_d, save_d, save_h, save_h, jax.ShapeDtypeStruct((8, 128), F32)),
            in_specs=[pl.BlockSpec(memory_space=pl.ANY)] * 4,
            out_specs=[pl.BlockSpec(memory_space=pl.ANY)] * 5,
            scratch_shapes=[
                pltpu.VMEM((4, 2, d_model, hidden), BF),
                pltpu.VMEM((6 * n_micro,) + piece, BF),
                pltpu.VMEM((3 * n_micro, n_tok, hidden), BF),
                pltpu.VMEM((2 * n_micro + 1, n_tok, hidden), BF),
                pltpu.VMEM((2 * nh,) + piece, BF),
                pltpu.VMEM((3 * nh,) + piece, BF),
                pltpu.VMEM((SR,) + piece, BF),
                pltpu.VMEM((SR,) + piece, BF),
                pltpu.VMEM((LB + 1,) + piece, F32),
                pltpu.VMEM((8, dpc), F32),
                pltpu.VMEM((2, 8, 128), F32),
                dma((6 * n_micro, NP)), dma((2 * nh, NP)), dma((3 * nh, NP)),
                dma((SR,)), dma((SR,)), dma((SR,)), dma((4,)), dma, dma((4,)), dma((16,)), dma((2,)),
                dma((2, 2, WCH)), dma, dma, dma, dma, pltpu.SemaphoreType.REGULAR,
            ],
            compiler_params=pltpu.CompilerParams(has_side_effects=True, vmem_limit_bytes=67043328),
            name="pipeline_step",
        )(x_loc, y_loc, w_in, w_out)
        grad_first = jnp.einsum("ktd,ktf->kdf", a_s, g_s, preferred_element_type=F32)[None]
        grad_second = jnp.einsum("ktf,ktd->kfd", z_s, d_s, preferred_element_type=F32)[None]
        return grad_first, grad_second, loss[0, :1]

    return jax.shard_map(
        device_program,
        mesh=mesh,
        in_specs=(P("dp", None, None), P("dp", None, None), P("pp", None, None, "tp"), P("pp", None, "tp", None)),
        out_specs=(P(("dp", "pp"), None, None, "tp"), P(("dp", "pp"), None, "tp", None), P("dp")),
        check_vma=False,
    )
```

```python
import functools
import math

import jax
import jax.numpy as jnp
from jax import lax
from jax.experimental import pallas as pl
from jax.experimental.pallas import tpu as pltpu
from jax.sharding import PartitionSpec as P

BF = jnp.bfloat16
F32 = jnp.float32
NP = 2
FB, BB, EF, EB = 4, 8, 4, 8
LB, LC = 1, 3
SR = 4
WCH = 8
GC = math.sqrt(2.0 / math.pi)
NT = (((1,), (1,)), ((), ()))
MESH = pl.DeviceIdType.MESH


def gelu_f(x):
    return x * (0.5 + 0.5 * jnp.tanh(GC * (x + 0.044715 * (x * x * x))))


def gelu_d(x):
    x2 = x * x
    th = jnp.tanh(GC * (x + 0.044715 * (x * x2)))
    return 0.5 + 0.5 * th + (0.5 * x) * (1.0 - th * th) * (GC + (3 * 0.044715 * GC) * x2)


def step_kernel(n_micro, inv_count, x_hbm, t_hbm, w1_hbm, w2_hbm,
                a_out, d_out, g_out, z_out, loss_out,
                w, act, ubuf, zbuf, pbuf, qbuf, sbuf, obuf, own, lacc, ltile,
                asem, psem, qsem, ssem, oesem, oosem, ldsem, tsem, outsem, lsend, lrecv,
                wrsem, wssem, wfsem, shsem, pxsem, gosem):
    nh = n_micro // 2
    n_tok, dpc = act.shape[2:]
    hid = ubuf.shape[2]
    nd = 3 * n_micro
    rows_w = w.shape[2] // WCH
    stage = lax.axis_index("pp")
    z = lax.axis_index("tp")
    x = lax.axis_index("dp")
    y = stage // 2
    core = lax.rem(stage, 2)
    y0, y1 = y == 0, y == 1
    c0, c1 = core == 0, core == 1
    mirror = lax.rem(stage + 2, 4)
    is_mid = (z == 1) | (z == 2)
    is_end = jnp.logical_not(is_mid)
    partner = z + 1 - 2 * lax.rem(z, 2)
    other = 3 - z
    n_slots = n_micro + 15 * nh

    def rcopy(src, dst, s_sem, r_sem, tp, pp):
        return pltpu.make_async_remote_copy(src_ref=src, dst_ref=dst, send_sem=s_sem, recv_sem=r_sem,
                                            device_id={"tp": tp, "pp": pp}, device_id_type=MESH)

    def wait_in(ref, sem):
        pltpu.make_async_copy(ref, ref, sem).wait()

    def decode(n):
        nn = jnp.maximum(n - n_micro, 0)
        r0 = n < n_micro
        rho = jnp.where(r0, 0, 1 + nn // nh)
        ext = n < nh
        j = jnp.where(r0, jnp.where(ext, n, n - nh), lax.rem(nn, nh))
        m = jnp.where(r0, jnp.where(ext, n + nh, n - nh), nh * y + j)
        fwd = rho < 8
        l = jnp.where(fwd, rho, 15 - rho)
        ok = (n >= 0) & (n < n_slots) & (lax.rem(l // 2, 2) == core)
        ok = ok & (y0 | ((rho > 0) & (rho < 15)))
        return dict(n=n, rho=rho, j=j, ext=ext, m=m, fwd=fwd, l=l, ok=ok, ar=ok & (rho < 15))

    def index_of(l, m, j, yy):
        home = (l // 4) == yy
        return jnp.where(home, lax.rem(l, 2) * n_micro + m, 2 * n_micro + lax.rem(l, 2) * nh + j)

    def p_slot(e):
        return jnp.where(e["ext"], nh + e["j"], e["j"])

    def q_slot(e):
        return jnp.where(e["ext"], 2 * nh + e["j"], lax.rem(e["rho"], 2) * nh + e["j"])

    def dest(e):
        l, m, j, fwd = e["l"], e["m"], e["j"], e["fwd"]
        last = fwd & (l == 7)
        dl = jnp.where(fwd, jnp.where(last, 7, l + 1), l - 1)
        dy = jnp.where(e["ext"], 1, jnp.where(jnp.logical_not(fwd) & (l == 1), 0, y))
        dc = lax.rem(dl // 2, 2)
        grad = last | jnp.logical_not(fwd)
        di = index_of(dl, m, j, dy) + jnp.where(grad, nd, 0)
        across = e["ext"] | (y1 & jnp.logical_not(fwd) & (l == 1))
        return last, di, 2 * dy + dc, (dy == y) & (dc == core), across

    loads = []
    for k in range(2):
        loads.append(pltpu.make_async_copy(w1_hbm.at[0, k], w.at[2 * y + k, 0], ldsem.at[k]))
        loads.append(pltpu.make_async_copy(w2_hbm.at[0, k], w.at[2 * y + k, 1], ldsem.at[2 + k]))
    for ld in loads:
        ld.start()

    @pl.when(y0 & c0)
    def _():
        @pl.loop(0, n_micro)
        def _(m):
            for c in range(NP):
                pltpu.make_async_copy(x_hbm.at[m, :, pl.ds(c * dpc, dpc)], act.at[m, c], asem.at[m, c]).start()

    lacc[...] = jnp.zeros_like(lacc)
    t_base = nd + index_of(7, nh * y, 0, y)

    @pl.when(c1 & is_mid)
    def _():
        @pl.loop(0, nh)
        def _(j):
            for c in range(NP):
                pltpu.make_async_copy(t_hbm.at[nh * y + j, :, pl.ds(c * dpc, dpc)], act.at[t_base + j, c], tsem).start()
        wait_in(act.at[pl.ds(t_base, nh)], tsem)

    for ld in loads:
        ld.wait()

    def send_weights(k):
        for i in range(WCH):
            half, g = i // (WCH // 2), lax.rem(2 * i, WCH) + x
            src = w.at[2 * y + k, half, pl.ds(g * rows_w, rows_w)]
            rcopy(src, src, wssem, wrsem.at[k, half, g], z, mirror).start()

    pl.when(jnp.logical_not(y0))(functools.partial(send_weights, 0))
    pl.when(c0 | y1)(functools.partial(send_weights, 1))

    @pl.when(y0 & c1)
    def _():
        pl.semaphore_wait(gosem, 1)
        send_weights(0)
        send_weights(1)

    n_chunk = jnp.where(y1 & c0, WCH, 2 * WCH)
    relay0 = jnp.where(y0, jnp.where(c0, 2, 26), jnp.where(c0, 0, 8))

    def relayed(n):
        late = jnp.where(n < 19, jnp.clip(n - relay0, 0, WCH), jnp.where(n < 24, n - 11, 2 * WCH))
        slow = jnp.clip((n - 4) // 2, 0, n_chunk)
        return jnp.where(y1 & c1 & (n > 8), late, jnp.where(y0 & c0, slow, jnp.clip(n - relay0, 0, n_chunk)))

    def relay(i):
        k = jnp.where(y1 & c0, 1, i // WCH)
        i = lax.rem(i, WCH)
        half = i // (WCH // 2)
        g = lax.rem(2 * i, WCH) + x
        ref = w.at[2 * (1 - y) + k, half, pl.ds(pl.multiple_of(g * rows_w, rows_w), rows_w)]
        wait_in(ref, wrsem.at[k, half, g])
        pltpu.make_async_remote_copy(src_ref=ref, dst_ref=ref, send_sem=wfsem, recv_sem=wrsem.at[k, half, g],
                                     device_id={"dp": 1 - x}, device_id_type=MESH).start()

    def wait_weights(k):
        for i in range(WCH):
            half, g = i // (WCH // 2), lax.rem(2 * i, WCH) + (1 - x)
            ref = w.at[2 * (1 - y) + k, half, pl.ds(pl.multiple_of(g * rows_w, rows_w), rows_w)]
            wait_in(ref, wrsem.at[k, half, g])

    def load_full(ai):
        return jnp.concatenate([act[ai, c] for c in range(NP)], axis=1)

    def put_act(ai, k, m, dst, sem):
        for c in range(NP):
            pltpu.make_async_copy(act.at[ai, c], dst.at[k, pl.ds(pl.multiple_of(m * n_tok, n_tok), n_tok), pl.ds(c * dpc, dpc)], sem).start()

    def put_hid(src, k, m, dst, sem):
        pltpu.make_async_copy(src, dst.at[k, pl.ds(pl.multiple_of(m * n_tok, n_tok), n_tok)], sem).start()

    def ship(ai, hi):
        rcopy(act.at[ai], act.at[hi], shsem, asem.at[hi, 0], z, mirror).start()

    def up_fwd(ai, wi, zi):
        a = load_full(ai)
        hb = hid // FB
        for n in range(FB):
            cs = pl.ds(n * hb, hb)
            u = jnp.dot(a, w[wi, 0, :, cs], preferred_element_type=F32).astype(BF)
            ubuf[ai, :, cs] = u
            zbuf[zi, :, cs] = gelu_f(u.astype(F32)).astype(BF)

    def up_bwd(ai, wi):
        d = load_full(nd + ai)
        hb = hid // BB
        for n in range(BB):
            cs = pl.ds(n * hb, hb)
            up = lax.dot_general(d, w[wi, 1, cs, :], NT, preferred_element_type=F32)
            ubuf[ai, :, cs] = (gelu_d(ubuf[ai, :, cs].astype(F32)) * up).astype(BF)

    def emit(e, nb, product):
        bw, per = dpc * NP // nb, nb // NP
        for c in range(NP):
            parts = [product(pl.ds((c * per + i) * bw, bw)) for i in range(per)]

            @pl.when(is_end)
            def _():
                s, r = lax.rem(e["n"], SR), p_slot(e)
                for i, part in enumerate(parts):
                    sbuf[s, c, :, pl.ds(i * bw, bw)] = part.astype(BF)
                rcopy(sbuf.at[s, c], pbuf.at[r, c], ssem.at[s], psem.at[r, c], partner, stage).start()

            @pl.when(is_mid)
            def _():
                for i, part in enumerate(parts):
                    own[lax.rem(e["n"], LB + 1), c, :, pl.ds(i * bw, bw)] = part

    def do_a(e):
        l, m, j, fwd = e["l"], e["m"], e["j"], e["fwd"]
        k = lax.rem(l, 2)
        home = (l // 4) == y
        wi = 2 * (l // 4) + k
        ai = index_of(l, m, j, y)
        hi = k * n_micro + m
        odd = k == 1

        @pl.when(fwd)
        def _():
            @pl.when(is_end | (k == 0) | ((l == 1) & y1))
            def _():
                for c in range(NP):
                    wait_in(act.at[ai, c], asem.at[ai, c])

                    @pl.when(is_mid & (l == 1))
                    def _():
                        rcopy(act.at[ai, c], act.at[ai, c], pxsem, asem.at[ai, c], partner, stage).start()

            @pl.when(jnp.logical_not(home))
            def _():
                ship(ai, hi)
                pl.when(j == 0)(functools.partial(wait_weights, k))

            zi = jnp.where(home, hi, 2 * n_micro)
            up_fwd(ai, wi, zi)

            @pl.when(home)
            def _():
                put_act(ai, k, m, a_out, outsem.at[0])
                put_hid(zbuf.at[zi], k, m, z_out, outsem.at[2])

            zz = zbuf[zi]
            emit(e, EF, lambda cs: jnp.dot(zz, w[wi, 1, :, cs], preferred_element_type=F32))

        @pl.when(jnp.logical_not(fwd))
        def _():
            @pl.when(is_end | (odd & (l < 7)))
            def _():
                for c in range(NP):
                    wait_in(act.at[nd + ai, c], asem.at[nd + ai, c])

            pl.when(jnp.logical_not(home))(functools.partial(ship, nd + ai, nd + hi))
            up_bwd(ai, wi)

            @pl.when(home)
            def _():
                put_act(nd + ai, k, m, d_out, outsem.at[1])
                put_hid(ubuf.at[ai], k, m, g_out, outsem.at[3])

            @pl.when(e["ar"])
            def _():
                gg = ubuf[ai]
                emit(e, EB, lambda cs: lax.dot_general(gg, w[wi, 0, cs, :], NT, preferred_element_type=F32))

    def do_b(e):
        s, r, qr = lax.rem(e["n"], SR), p_slot(e), q_slot(e)
        so = lax.rem(e["n"], LB + 1)
        for c in range(NP):
            wait_in(pbuf.at[r, c], psem.at[r, c])
            sbuf[s, c] = (own[so, c] + pbuf[r, c].astype(F32)).astype(BF)
            rcopy(sbuf.at[s, c], qbuf.at[qr, c], ssem.at[s], qsem.at[qr, c], other, stage).start()

    def do_c(e):
        s, qr = lax.rem(e["n"], SR), q_slot(e)
        ai = index_of(e["l"], e["m"], e["j"], y) + jnp.where(e["fwd"], 0, nd)
        last, di, ds, local, across = dest(e)
        for c in range(NP):
            wait_in(qbuf.at[qr, c], qsem.at[qr, c])
            h = act[ai, c].astype(F32) + (sbuf[s, c].astype(F32) + qbuf[qr, c].astype(F32))
            h = h.astype(BF)

            @pl.when(last)
            def _():
                err = h.astype(F32) - act[di, c].astype(F32)
                lacc[...] += jnp.sum((err * err).reshape(n_tok // 8, 8, dpc), axis=0)
                dy = (err * inv_count).astype(BF)
                obuf[s, c] = dy
                act[di, c] = dy

            @pl.when(jnp.logical_not(last))
            def _():
                obuf[s, c] = h

                @pl.when(local)
                def _():
                    act[di, c] = h

            @pl.when(jnp.logical_not(local))
            def _():
                rcopy(obuf.at[s, c], act.at[di, c], oosem.at[s], asem.at[di, c], z, ds).start()

            @pl.when(jnp.logical_not(across))
            def _():
                rcopy(obuf.at[s, c], act.at[di, c], oesem.at[s], asem.at[di, c], partner, ds).start()

    redo_b0 = jnp.where(y0, jnp.where(c0, n_slots - nh, n_slots - 2 * nh), jnp.where(c0, n_slots - 4 * nh, n_slots - 6 * nh))
    redo_f0 = jnp.where(y0, jnp.where(c0, n_slots - 9 * nh, n_slots - 6 * nh), jnp.where(c0, n_slots - 8 * nh, n_slots - 6 * nh))
    n_redo_f = jnp.where(y0 & c0, nh, 2 * nh)

    def redo_at(i):
        k = 1 - i // nh
        m = nh * (1 - y) + lax.rem(i, nh)
        return k, m, k * n_micro + m, 2 * y + k

    def redo_f(i):
        k, m, hi, wi = redo_at(i)
        wait_in(act.at[hi], asem.at[hi, 0])
        put_act(hi, k, m, a_out, outsem.at[0])
        up_fwd(hi, wi, hi)
        put_hid(zbuf.at[hi], k, m, z_out, outsem.at[2])

    def redo_b(i):
        k, m, hi, wi = redo_at(i)
        layer0 = y0 & c0 & (k == 0)

        @pl.when(jnp.logical_not(layer0))
        def _():
            wait_in(act.at[nd + hi], asem.at[nd + hi, 0])

        @pl.when(layer0)
        def _():
            for c in range(NP):
                wait_in(act.at[nd + hi, c], asem.at[nd + hi, c])

                @pl.when(is_mid)
                def _():
                    rcopy(act.at[nd + hi, c], act.at[nd + hi, c], pxsem, asem.at[nd + hi, c], partner, stage).start()

        put_act(nd + hi, k, m, d_out, outsem.at[1])
        up_bwd(hi, wi)
        put_hid(ubuf.at[hi], k, m, g_out, outsem.at[3])

    def slot(n, carry):
        e = decode(n)
        old = decode(n - SR)
        eb, ebo = decode(n - LB), decode(n - LB - SR)
        ec, eco = decode(n - LC), decode(n - LC - SR)

        @pl.when((is_end & old["ar"]) | (is_mid & ebo["ar"]))
        def _():
            s = lax.rem(n + SR - jnp.where(is_end, 0, LB), SR)
            wait_in(sbuf.at[s], ssem.at[s])

        @pl.when(is_mid & eco["ar"])
        def _():
            s = lax.rem(n + SR - LC, SR)
            local, across = dest(eco)[3:]
            pl.when(jnp.logical_not(across))(lambda: wait_in(obuf.at[s], oesem.at[s]))
            pl.when(jnp.logical_not(local))(lambda: wait_in(obuf.at[s], oosem.at[s]))

        @pl.loop(relayed(n), relayed(n + 1))
        def _(i):
            relay(i)

        pl.when(e["ok"])(functools.partial(do_a, e))
        pl.when(is_mid & ec["ar"])(functools.partial(do_c, ec))
        pl.when(is_mid & eb["ar"])(functools.partial(do_b, eb))

        @pl.when(y0 & c0 & (n == 6))
        def _():
            wait_in(w.at[1, 0], wssem)
            pl.semaphore_signal(gosem, 1, device_id={"pp": 1}, device_id_type=MESH)

        fi = n - redo_f0
        pl.when((fi >= 0) & (fi < n_redo_f))(functools.partial(redo_f, fi))
        bi = n - redo_b0
        pl.when((bi >= 0) & (bi < 2 * nh))(functools.partial(redo_b, bi))
        return carry

    lax.fori_loop(0, n_slots + LC + SR + 2, slot, 0)

    owner = (z == 1) & c1

    @pl.when(owner)
    def _():
        ltile[y] = jnp.full(ltile.shape[1:], jnp.sum(lacc[...]) * inv_count * 0.5, F32)
        for i in range(16):
            tp, pp = i // 4, i % 4

            @pl.when((tp != 1) | (pp != stage))
            def _():
                rcopy(ltile.at[y], ltile.at[y], lsend.at[i], lrecv.at[y], tp, pp).start()
        for i in range(16):
            tp, pp = i // 4, i % 4

            @pl.when((tp != 1) | (pp != stage))
            def _():
                wait_in(ltile.at[y], lsend.at[i])

    for yy in range(2):
        @pl.when(jnp.logical_not(owner & (y == yy)))
        def _():
            wait_in(ltile.at[yy], lrecv.at[yy])

    ltile[0] = ltile[0] + ltile[1]
    lout = pltpu.make_async_copy(ltile.at[0], loss_out, tsem)
    lout.start()
    lout.wait()

    for full, sem in ((jnp.logical_not(y0 & c0), wssem), (jnp.logical_not(y1 & c0), wfsem)):
        pl.when(full)(functools.partial(wait_in, w.at[0], sem))
    pl.when(y1 & c0)(functools.partial(wait_in, w.at[0, 0], wfsem))
    pl.when(c0 & is_mid)(functools.partial(wait_in, act.at[pl.ds(0, nh)], pxsem))
    half_ship = y1 & c0
    pl.when(half_ship)(functools.partial(wait_in, act.at[pl.ds(0, n_micro)], shsem))
    pl.when(jnp.logical_not(half_ship))(functools.partial(wait_in, act.at[pl.ds(0, 2 * n_micro)], shsem))
    pltpu.make_async_copy(a_out, a_out, outsem.at[0]).wait()
    pltpu.make_async_copy(d_out, d_out, outsem.at[1]).wait()
    pltpu.make_async_copy(z_out, z_out, outsem.at[2]).wait()
    pltpu.make_async_copy(g_out, g_out, outsem.at[3]).wait()


def solution(mesh):
    assert (mesh.shape["tp"], mesh.shape["pp"], mesh.shape["dp"]) == (4, 4, 2)

    def device_program(x_loc, y_loc, w_in, w_out):
        n_micro, n_tok, d_model = x_loc.shape
        hidden = w_in.shape[3]
        assert d_model == hidden and n_micro % 2 == 0
        dpc = d_model // NP
        nh = n_micro // 2
        inv_count = 1.0 / (n_micro * n_tok * d_model)
        rows = n_micro * n_tok
        save_d = jax.ShapeDtypeStruct((2, rows, d_model), BF)
        save_h = jax.ShapeDtypeStruct((2, rows, hidden), BF)
        dma = pltpu.SemaphoreType.DMA
        piece = (NP, n_tok, dpc)
        a_s, d_s, g_s, z_s, loss = pl.pallas_call(
            functools.partial(step_kernel, n_micro, inv_count),
            out_shape=(save_d, save_d, save_h, save_h, jax.ShapeDtypeStruct((8, 128), F32)),
            in_specs=[pl.BlockSpec(memory_space=pl.ANY)] * 4,
            out_specs=[pl.BlockSpec(memory_space=pl.ANY)] * 5,
            scratch_shapes=[
                pltpu.VMEM((4, 2, d_model, hidden), BF),
                pltpu.VMEM((6 * n_micro,) + piece, BF),
                pltpu.VMEM((3 * n_micro, n_tok, hidden), BF),
                pltpu.VMEM((2 * n_micro + 1, n_tok, hidden), BF),
                pltpu.VMEM((2 * nh,) + piece, BF),
                pltpu.VMEM((3 * nh,) + piece, BF),
                pltpu.VMEM((SR,) + piece, BF),
                pltpu.VMEM((SR,) + piece, BF),
                pltpu.VMEM((LB + 1,) + piece, F32),
                pltpu.VMEM((8, dpc), F32),
                pltpu.VMEM((2, 8, 128), F32),
                dma((6 * n_micro, NP)), dma((2 * nh, NP)), dma((3 * nh, NP)),
                dma((SR,)), dma((SR,)), dma((SR,)), dma((4,)), dma, dma((4,)), dma((16,)), dma((2,)),
                dma((2, 2, WCH)), dma, dma, dma, dma, pltpu.SemaphoreType.REGULAR,
            ],
            compiler_params=pltpu.CompilerParams(has_side_effects=True, vmem_limit_bytes=67043328),
            name="pipeline_step",
        )(x_loc, y_loc, w_in, w_out)
        grad_first = jnp.einsum("ktd,ktf->kdf", a_s, g_s, preferred_element_type=F32)[None]
        grad_second = jnp.einsum("ktf,ktd->kfd", z_s, d_s, preferred_element_type=F32)[None]
        return grad_first, grad_second, loss[0, :1]

    return jax.shard_map(
        device_program,
        mesh=mesh,
        in_specs=(P("dp", None, None), P("dp", None, None), P("pp", None, None, "tp"), P("pp", None, "tp", None)),
        out_specs=(P(("dp", "pp"), None, None, "tp"), P(("dp", "pp"), None, "tp", None), P("dp")),
        check_vma=False,
    )
```
